256 devices in a mesh: task: 4 (over z_lo), tile: 64 (over y, z_hi, x, core).
Axes of the slice: x: 4, y: 4, z: 8 (z_hi: 2, z_lo: 4; z = z_hi * 4 + z_lo), core: 2. Of those that a mesh axis runs over, the one named last changes fastest.
Arguments:
- adjusted: bfloat16 [8, 3584, 18944], P('task', 'tile'), may hold values from -6 to 6
- fisher: bfloat16 [8, 3584, 18944], P('task', 'tile'), may hold values from 0.0099487305 to 10
Outputs:
- merged: bfloat16 [3584, 18944], P(None, ('task', 'tile'))
The draws below stay inside these ranges and needn't reach their ends.
All inputs are finite; a program needn't handle non-finite values.
Results may differ from the reference program's by a relative error of at most 0.001.
Values may be sent and summed in bfloat16 or wider, within the bound.
No kernel may reach another device: no remote copies, remote signals or barrier semaphores. Data moves between devices by JAX's collectives and lax.ppermute only.
A program may use at most 64 MiB of HBM per device.

```python
import math
import jax
import jax.numpy as jnp
from jax import lax

D = 3584
FF = 18944
MODELS = 8


def level_of(own_key, extent, cuts, least, top_value):
    def one(position, shards_of):
        steps = jax.random.uniform(jax.random.fold_in(jax.random.fold_in(own_key, 6), position), (shards_of,), jnp.float32, least / len(cuts), top_value / len(cuts))
        return jnp.repeat(jnp.exp(steps), extent[position] // shards_of).reshape((-1,) + (1,) * (len(extent) - position - 1))

    factor_of = one(*cuts[0])
    for cut in cuts[1:]:
        factor_of = factor_of * one(*cut)
    return factor_of


def gaussian(stream_key, dims, width, most, shards=(), dtype=jnp.bfloat16):
    array = width * jax.random.normal(stream_key, dims, jnp.float32)
    if shards:
        array = array * level_of(stream_key, dims, shards, -0.22, 0.18)
    return jnp.clip(array, -most, most).astype(dtype)


def setup_inputs(seed: int = 0) -> dict:
    keys = jax.random.split(jax.random.key(seed), 3)
    adjusted = gaussian(keys[0], (MODELS, D, FF), 1.0, 6.0, ((0, 4), (1, 64)))
    fisher = jnp.clip(jnp.exp(math.log(10.0) - 6.912895 * jax.random.uniform(keys[1], (MODELS, D, FF), jnp.float32) ** level_of(keys[1], (MODELS, D, FF), ((0, 4), (1, 64)), -0.2, 0.2)), 0.0099487305, 10.0).astype(jnp.bfloat16)
    return dict(adjusted=adjusted, fisher=fisher)


def reference(adjusted, fisher):
    def accumulate(carry, pair):
        numerator, denominator = carry
        weights, curvature = pair
        scaled = curvature.astype(jnp.float32)
        return (numerator + scaled * weights.astype(jnp.float32), denominator + scaled), None

    zeros = jnp.zeros((D, FF), jnp.float32)
    (numerator, denominator), unused = lax.scan(accumulate, (zeros, zeros), (adjusted, fisher))
    return (numerator / denominator).astype(jnp.bfloat16)
```

```python
import functools

import jax
import jax.numpy as jnp
from jax import lax
from jax.experimental import pallas as pl
from jax.experimental.pallas import tpu as pltpu
from jax.sharding import PartitionSpec as P

ROWS = (56,)
LANES = 128
SUB = 8

TOP = 6.0
M_SCALE = 251.0 / TOP
M_BASE = -125.0
LOG_LOW = -6.0
LOG_HIGH = 6.5
D_SCALE = 250.0 / (LOG_HIGH - LOG_LOW)
D_BASE = -125.0 - D_SCALE * LOG_LOW


def encode(n, d):
    m = n / d
    y = jnp.exp2(jnp.abs(m) * M_SCALE + M_BASE)
    y = jnp.where(m < 0, -y, y)
    z = jnp.exp2(jnp.log2(d) * D_SCALE + D_BASE)
    return y.astype(jnp.bfloat16), z.astype(jnp.bfloat16)


def decode(y, z):
    y = y.astype(jnp.float32)
    m = (jnp.log2(jnp.abs(y)) - M_BASE) * (1.0 / M_SCALE)
    m = jnp.where(y < 0, -m, m)
    d = jnp.exp2((jnp.log2(z.astype(jnp.float32)) - D_BASE) * (1.0 / D_SCALE))
    return m * d, d


def local(a_ref, f_ref, at):
    n = d = None
    for m in range(a_ref.shape[0]):
        f = f_ref[m, :, at].astype(jnp.float32)
        p = f * a_ref[m, :, at].astype(jnp.float32)
        n, d = (p, f) if n is None else (n + p, d + f)
    return n, d


def tiles(width):
    return [slice(c, c + LANES) for c in range(0, width, LANES)]


def first_kernel(q_ref, a_ref, f_ref, o_ref):
    for at in tiles(a_ref.shape[2]):
        o_ref[0, 0, :, at], o_ref[0, 1, :, at] = encode(*local(a_ref, f_ref, at))


def second_kernel(q_ref, a_ref, f_ref, r_ref, o_ref):
    for at in tiles(a_ref.shape[2]):
        n, d = local(a_ref, f_ref, at)
        rn, rd = decode(r_ref[0, 0, :, at], r_ref[0, 1, :, at])
        o_ref[0, :, at], o_ref[1, :, at] = encode(n + rn, d + rd)


def third_kernel(q_ref, a_ref, f_ref, r_ref, s_ref, o_ref, w_ref):
    for at in tiles(a_ref.shape[2]):
        n, d = local(a_ref, f_ref, at)
        rn, rd = decode(r_ref[0, 0, :, at], r_ref[0, 1, :, at])
        sn, sd = decode(s_ref[0, :, at], s_ref[1, :, at])
        w_ref[:, at] = (n + rn + sn) / (d + rd + sd)
    peers, _, cols = o_ref.shape
    for j in range(peers):
        o_ref[j] = w_ref[:, j * cols : (j + 1) * cols].astype(jnp.bfloat16)


def call(kernel, grid, quarters, in_specs, out_specs, out_shape, scratch, *args):
    return pl.pallas_call(
        kernel,
        grid_spec=pltpu.PrefetchScalarGridSpec(
            num_scalar_prefetch=1, grid=grid, in_specs=in_specs, out_specs=out_specs, scratch_shapes=scratch
        ),
        out_shape=out_shape,
    )(quarters, *args)


def body(tile, adjusted, fisher):
    models, rows, width = adjusted.shape
    part = width // 4
    bf16 = jnp.bfloat16
    t = lax.axis_index("task")
    pick = lambda *xs: jnp.stack([t ^ x for x in xs]).astype(jnp.int32)
    outs, start = [], 0
    for r in ROWS:
        at = start // SUB
        start += r
        n = r // SUB
        raw2 = pl.BlockSpec((models, SUB, part), lambda s, i, q, at=at: (0, at + i, q[s]))
        raw1 = pl.BlockSpec((models, SUB, part), lambda i, q, at=at: (0, at + i, q[0]))
        pair = pl.BlockSpec((2, SUB, part), lambda i, q: (0, i, 0))
        slot = lambda k: pl.BlockSpec((1, 2, SUB, part), lambda i, q: (k, 0, i, 0))
        sent = call(
            first_kernel, (2, n), pick(1, 3), [raw2, raw2],
            pl.BlockSpec((1, 2, SUB, part), lambda s, i, q: (s, 0, i, 0)),
            jax.ShapeDtypeStruct((2, 2, r, part), bf16), [], adjusted, fisher,
        )
        got = lax.ppermute(sent, "task", [(k, k ^ 1) for k in range(4)])
        sent = call(
            second_kernel, (n,), pick(2), [raw1, raw1, slot(1)], pair,
            jax.ShapeDtypeStruct((2, r, part), bf16), [], adjusted, fisher, got,
        )
        last = lax.ppermute(sent, "task", [(k, k ^ 2) for k in range(4)])
        cols = part // tile
        merged = call(
            third_kernel, (n,), pick(0), [raw1, raw1, slot(0), pair],
            pl.BlockSpec((tile, SUB, cols), lambda i, q: (0, i, 0)),
            jax.ShapeDtypeStruct((tile, r, cols), bf16), [pltpu.VMEM((SUB, part), jnp.float32)],
            adjusted, fisher, got, last,
        )
        outs.append(lax.all_to_all(merged, "tile", 0, 0, tiled=True))
    out = jnp.concatenate(outs, axis=1) if len(outs) > 1 else outs[0]
    return out.reshape(tile * rows, part // tile)


def solution(mesh):
    return jax.shard_map(
        functools.partial(body, mesh.shape["tile"]),
        mesh=mesh,
        in_specs=(P("task", "tile", None), P("task", "tile", None)),
        out_specs=P(None, ("task", "tile")),
        check_vma=False,
    )
```

```python
import functools

import jax
import jax.numpy as jnp
from jax import lax
from jax.experimental import pallas as pl
from jax.experimental.pallas import tpu as pltpu
from jax.sharding import Mesh, PartitionSpec as P

ROWS = (24, 16, 16)
LANES = 128
SUB = 8
TILE = (("y", 4), ("half", 2), ("x", 4), ("core", 2))
PLANE = ("y", "x", "core")

TOP = 6.0
M_SCALE = 251.0 / TOP
M_BASE = -125.0
LOG_LOW = -6.0
LOG_HIGH = 6.5
D_SCALE = 250.0 / (LOG_HIGH - LOG_LOW)
D_BASE = -125.0 - D_SCALE * LOG_LOW


def encode(n, d):
    m = n / d
    y = jnp.exp2(jnp.abs(m) * M_SCALE + M_BASE)
    y = jnp.where(m < 0, -y, y)
    z = jnp.exp2(jnp.log2(d) * D_SCALE + D_BASE)
    return y.astype(jnp.bfloat16), z.astype(jnp.bfloat16)


def decode(y, z):
    y = y.astype(jnp.float32)
    m = (jnp.log2(jnp.abs(y)) - M_BASE) * (1.0 / M_SCALE)
    m = jnp.where(y < 0, -m, m)
    d = jnp.exp2((jnp.log2(z.astype(jnp.float32)) - D_BASE) * (1.0 / D_SCALE))
    return m * d, d


def sums(refs, segment, c):
    at = slice(c, c + LANES)
    first, last = c // segment, (c + LANES - 1) // segment

    def load(k, m):
        two = [refs[2 * (s % 2) + k][m, :, at].astype(jnp.float32) for s in sorted({first, last})]
        if len(two) == 1:
            return two[0]
        lane = lax.broadcasted_iota(jnp.int32, two[0].shape, 1)
        return jnp.where(lane < last * segment - c, two[0], two[1])

    n = d = None
    for m in range(refs[0].shape[0]):
        f = load(1, m)
        p = f * load(0, m)
        n, d = (p, f) if n is None else (n + p, d + f)
    return at, n, d


def first_kernel(segment, q_ref, a0, f0, a1, f1, o_ref):
    for c in range(0, a0.shape[2], LANES):
        at, n, d = sums((a0, f0, a1, f1), segment, c)
        o_ref[0, 0, :, at], o_ref[0, 1, :, at] = encode(n, d)


def second_kernel(segment, q_ref, a0, f0, a1, f1, r_ref, o_ref):
    for c in range(0, a0.shape[2], LANES):
        at, n, d = sums((a0, f0, a1, f1), segment, c)
        rn, rd = decode(r_ref[0, 0, :, at], r_ref[0, 1, :, at])
        o_ref[0, :, at], o_ref[1, :, at] = encode(n + rn, d + rd)


def third_kernel(segment, q_ref, a0, f0, a1, f1, r_ref, s_ref, o_ref, w_ref):
    for c in range(0, a0.shape[2], LANES):
        at, n, d = sums((a0, f0, a1, f1), segment, c)
        rn, rd = decode(r_ref[0, 0, :, at], r_ref[0, 1, :, at])
        sn, sd = decode(s_ref[0, :, at], s_ref[1, :, at])
        w_ref[:, at] = (n + rn + sn) / (d + rd + sd)
    halves, peers, _, cols = o_ref.shape
    per = segment // cols
    for j in range(halves * peers):
        block, k = divmod(j, per)
        to = w_ref[:, j * cols : (j + 1) * cols].astype(jnp.bfloat16)
        o_ref[block % 2, block // 2 * per + k] = to


def call(kernel, grid, quarters, in_specs, out_specs, out_shape, scratch, *args):
    return pl.pallas_call(
        kernel,
        grid_spec=pltpu.PrefetchScalarGridSpec(
            num_scalar_prefetch=1, grid=grid, in_specs=in_specs, out_specs=out_specs, scratch_shapes=scratch
        ),
        out_shape=out_shape,
    )(quarters, *args)


def body(adjusted, fisher):
    models, rows, width = adjusted.shape
    part = width // 4
    bf16 = jnp.bfloat16
    sizes = dict(TILE)
    peers = sizes["y"] * sizes["x"] * sizes["core"]
    cols = part // (2 * peers)
    segment = cols * sizes["x"] * sizes["core"]
    t = lax.axis_index("task")
    half = lax.axis_index("half")
    pick = lambda *xs: jnp.stack([t ^ x ^ jnp.where(half == h, 0, 3) for x in xs for h in (0, 1)]).astype(jnp.int32)
    raw = (adjusted, fisher, adjusted, fisher)
    outs, start = [], 0
    for r in ROWS:
        at = start // SUB
        start += r
        n = r // SUB
        raw2 = lambda k: pl.BlockSpec((models, SUB, part), lambda s, i, q: (0, at + i, q[2 * s + k]))
        raw1 = lambda k: pl.BlockSpec((models, SUB, part), lambda i, q: (0, at + i, q[k]))
        raws1 = [raw1(0), raw1(0), raw1(1), raw1(1)]
        pair = pl.BlockSpec((2, SUB, part), lambda i, q: (0, i, 0))
        slot = lambda k: pl.BlockSpec((1, 2, SUB, part), lambda i, q: (k, 0, i, 0))
        sent = call(
            functools.partial(first_kernel, segment), (2, n), pick(1, 3), [raw2(0), raw2(0), raw2(1), raw2(1)],
            pl.BlockSpec((1, 2, SUB, part), lambda s, i, q: (s, 0, i, 0)),
            jax.ShapeDtypeStruct((2, 2, r, part), bf16), [], *raw,
        )
        got = lax.ppermute(sent, "task", [(k, k ^ 1) for k in range(4)])
        sent = call(
            functools.partial(second_kernel, segment), (n,), pick(2), [*raws1, slot(1)], pair,
            jax.ShapeDtypeStruct((2, r, part), bf16), [], *raw, got,
        )
        last = lax.ppermute(sent, "task", [(k, k ^ 2) for k in range(4)])
        merged = call(
            functools.partial(third_kernel, segment), (n,), pick(0), [*raws1, slot(0), pair],
            pl.BlockSpec((2, peers, SUB, cols), lambda i, q: (0, 0, i, 0)),
            jax.ShapeDtypeStruct((2, peers, r, cols), bf16), [pltpu.VMEM((SUB, part), jnp.float32)],
            *raw, got, last,
        )
        own, other = (lax.select(half == 0, merged[k], merged[1 - k]) for k in (0, 1))
        other = lax.ppermute(other, ("task", "half"), [(2 * u + h, 2 * (u ^ 3) + 1 - h) for u in range(4) for h in (0, 1)])
        both = jnp.stack([lax.select(half == 0, own, other), lax.select(half == 0, other, own)], axis=1)
        outs.append(lax.all_to_all(both, PLANE, 0, 0, tiled=True))
    out = jnp.concatenate(outs, axis=2) if len(outs) > 1 else outs[0]
    out = out.reshape(sizes["y"], sizes["x"] * sizes["core"], 2, rows, cols).transpose(0, 2, 1, 3, 4)
    return out.reshape(2 * peers * rows, cols)


def solution(mesh):
    names, sizes = zip(*TILE)
    fine = Mesh(mesh.devices.reshape(mesh.shape["task"], *sizes), ("task", *names))
    return jax.shard_map(
        body,
        mesh=fine,
        in_specs=(P("task", names, None), P("task", names, None)),
        out_specs=P(None, ("task", *names)),
        check_vma=False,
    )
```
